32 devices in a mesh: gx: 4 (over z), gy: 4 (over x, core), gz: 2 (over y).
Axes of the slice: x: 2, y: 2, z: 4, core: 2. Of those that a mesh axis runs over, the one named last changes fastest.
Arguments:
- source: float32 [64, 32, 512], P('gx', 'gz', 'gy'), may hold values from -0.6 to 0.6
- shift: float32 [1], replicated, may hold values from 1e-05 to 0.0001
Outputs:
- solution: float32 [64, 32, 512], P('gx', 'gz', 'gy')
The draws below stay inside these ranges and needn't reach their ends.
All inputs are finite; a program needn't handle non-finite values.
Results may differ from the reference program's by a relative error of at most 0.0004.
Values sent between devices are 32-bit elements; how exact they have to be, the bound alone decides.
A program may use at most 64 MiB of HBM per device.

```python
import math
import jax
import jax.numpy as jnp
from jax import lax

LEVELS = 4
NU_PRE = 1
NU_POST = 1
N0 = 64
N1 = 32
N2 = 512


MEAN_LEVEL = 1e-06


def draw_source(key, part):
    rough_key = jax.random.fold_in(jax.random.fold_in(key, 11), 0)
    rough = jnp.clip(0.1 * jax.random.normal(rough_key, (N0, N1, N2), jnp.float32), -0.59, 0.59)
    return rough - jnp.mean(rough) + MEAN_LEVEL


def setup_inputs(seed: int = 0) -> dict:
    streams_of = jax.random.split(jax.random.key(seed), 3)
    source = draw_source(jax.random.fold_in(streams_of[2], 71), 0)
    shift = jnp.clip(jnp.exp(jax.random.uniform(streams_of[1], (1,), jnp.float32, math.log(9.999999747378752e-06), math.log(0.0001))), 9.999999747378752e-06, 0.0001)
    return {"source": source, "shift": shift}


DAMPING = 6.0 / 7.0
PRECISE = lax.Precision.HIGHEST
CUBIC_EVEN = (-5.0 / 128.0, 35.0 / 128.0, 105.0 / 128.0, -7.0 / 128.0)
CUBIC_ODD = (-7.0 / 128.0, 105.0 / 128.0, 35.0 / 128.0, -5.0 / 128.0)
LINEAR_EVEN = (0.25, 0.75)
LINEAR_ODD = (0.75, 0.25)


def wrapped(values, width):
    return jnp.pad(values, width, mode="wrap")


def neighbours(padded):
    center = padded[1:-1, 1:-1, 1:-1]
    beside_all = padded[2:, 1:-1, 1:-1] + padded[:-2, 1:-1, 1:-1]
    beside_all = beside_all + padded[1:-1, 2:, 1:-1] + padded[1:-1, :-2, 1:-1]
    beside_all = beside_all + padded[1:-1, 1:-1, 2:] + padded[1:-1, 1:-1, :-2]
    return center, beside_all


def defect(padded, forcing, weight_nb, diagonal):
    center, beside_all = neighbours(padded)
    return forcing - (diagonal * center - weight_nb * beside_all)


def relaxed(padded, forcing, weight_nb, diagonal):
    center, beside_all = neighbours(padded)
    return center + DAMPING * (forcing - (diagonal * center - weight_nb * beside_all)) / diagonal


def coarsen(values):
    values = values[0::2] + values[1::2]
    values = values[:, 0::2] + values[:, 1::2]
    values = values[:, :, 0::2] + values[:, :, 1::2]
    return 0.125 * values


def refine_axis(padded, dimension, even_weights, odd_weights):
    margin = len(even_weights) // 2
    length = padded.shape[dimension] - 2 * margin
    even_cells = even_weights[0] * lax.slice_in_dim(padded, 0, length, axis=dimension)
    odd_cells = odd_weights[0] * lax.slice_in_dim(padded, 1, 1 + length, axis=dimension)
    for offset in range(1, len(even_weights)):
        even_cells = even_cells + even_weights[offset] * lax.slice_in_dim(padded, offset, offset + length, axis=dimension)
        odd_cells = odd_cells + odd_weights[offset] * lax.slice_in_dim(padded, offset + 1, offset + 1 + length, axis=dimension)
    stacked = jnp.stack([even_cells, odd_cells], axis=dimension + 1)
    new_shape = list(even_cells.shape)
    new_shape[dimension] = 2 * length
    return stacked.reshape(new_shape)


def refine(padded, even_weights, odd_weights):
    for dimension in range(3):
        padded = refine_axis(padded, dimension, even_weights, odd_weights)
    return padded


def tables(cells_count):
    indices = jnp.arange(cells_count, dtype=jnp.int32)
    angles = ((indices[:, None] * indices[None, :]) % cells_count).astype(jnp.float32) * (2.0 * math.pi / cells_count)
    return jnp.cos(angles), jnp.sin(angles)


def along_axis(matrix, values, dimension):
    product = jnp.tensordot(matrix, values, axes=([1], [dimension]), precision=PRECISE)
    return jnp.moveaxis(product, 0, dimension)


def coarse_solve(forcing, shift_value, weight_nb):
    cosine_table, sine_table = tables(forcing.shape[0])
    real_part = along_axis(cosine_table, forcing, 0)
    imag_part = -along_axis(sine_table, forcing, 0)
    for dimension in (1, 2):
        cosine_table, sine_table = tables(forcing.shape[dimension])
        real_next = along_axis(cosine_table, real_part, dimension) + along_axis(sine_table, imag_part, dimension)
        imag_part = along_axis(cosine_table, imag_part, dimension) - along_axis(sine_table, real_part, dimension)
        real_part = real_next
    cosines = [jnp.cos(jnp.arange(cells_count, dtype=jnp.float32) * (2.0 * math.pi / cells_count)) for cells_count in forcing.shape]
    eigenvalue = weight_nb * (6.0 - 2.0 * cosines[0][:, None, None] - 2.0 * cosines[1][None, :, None] - 2.0 * cosines[2][None, None, :]) + shift_value
    real_part = real_part / eigenvalue
    imag_part = imag_part / eigenvalue
    for dimension in (0, 1):
        cosine_table, sine_table = tables(forcing.shape[dimension])
        real_next = along_axis(cosine_table, real_part, dimension) - along_axis(sine_table, imag_part, dimension)
        imag_part = along_axis(cosine_table, imag_part, dimension) + along_axis(sine_table, real_part, dimension)
        real_part = real_next
    cosine_table, sine_table = tables(forcing.shape[2])
    real_part = along_axis(cosine_table, real_part, 2) - along_axis(sine_table, imag_part, 2)
    return real_part / float(forcing.size)


def vcycle(grid_level, iterate, forcing, shift_value):
    weight_nb = 0.25 ** grid_level
    diagonal = 6.0 * weight_nb + shift_value
    for sweep_index in range(NU_PRE):
        iterate = relaxed(wrapped(iterate, 1), forcing, weight_nb, diagonal)
    residue = coarsen(defect(wrapped(iterate, 1), forcing, weight_nb, diagonal))
    if grid_level + 1 == LEVELS - 1:
        correction = coarse_solve(residue, shift_value, 0.25 ** (grid_level + 1))
    else:
        correction = vcycle(grid_level + 1, jnp.zeros_like(residue), residue, shift_value)
    iterate = iterate + refine(wrapped(correction, 1), LINEAR_EVEN, LINEAR_ODD)
    for sweep_index in range(NU_POST):
        iterate = relaxed(wrapped(iterate, 1), forcing, weight_nb, diagonal)
    return iterate


def reference(source, shift):
    shift_value = shift[0]
    sources = [source]
    for grid_level in range(1, LEVELS):
        sources.append(coarsen(sources[-1]))
    iterate = coarse_solve(sources[-1], shift_value, 0.25 ** (LEVELS - 1))
    for grid_level in range(LEVELS - 2, -1, -1):
        iterate = refine(wrapped(iterate, 2), CUBIC_EVEN, CUBIC_ODD)
        iterate = vcycle(grid_level, iterate, sources[grid_level], shift_value)
    return iterate
```

```python
import functools

import jax
import jax.numpy as jnp
import numpy as np
from jax import lax
from jax.experimental import pallas as pl
from jax.experimental.pallas import tpu as pltpu
from jax.sharding import PartitionSpec as P

LEVELS = 4
DAMPING = 6.0 / 7.0
PRECISE = lax.Precision.HIGHEST
CUBIC = (
    {-2: -5.0 / 128.0, -1: 35.0 / 128.0, 0: 105.0 / 128.0, 1: -7.0 / 128.0},
    {-1: -7.0 / 128.0, 0: 105.0 / 128.0, 1: 35.0 / 128.0, 2: -5.0 / 128.0},
)
LINEAR = ({-1: 0.25, 0: 0.75}, {0: 0.75, 1: 0.25})
NAMES = ("gx", "gy", "gz")


def basis(count):
    cells = np.arange(count)
    columns, cosines = [], []
    for m in range(count):
        k = (m + 1) // 2
        angle = 2.0 * np.pi * k * cells / count
        column = np.cos(angle) if m % 2 == 1 or m == 0 else np.sin(angle)
        columns.append(column / np.sqrt(np.sum(column**2)))
        cosines.append(np.cos(2.0 * np.pi * k / count))
    return np.stack(columns, axis=1), np.array(cosines, np.float32)


def interpolation(coarse_count, fine_cells, weights):
    matrix = np.zeros((len(fine_cells), coarse_count))
    for row, cell in enumerate(fine_cells):
        for offset, weight in weights[cell % 2].items():
            matrix[row, (cell // 2 + offset) % coarse_count] += weight
    return matrix


def pairs(coarse_count):
    return np.kron(np.eye(coarse_count), np.ones((1, 2)))


def blocked(matrix):
    count = max(1, 128 // matrix.shape[1])
    return np.kron(np.eye(count), matrix)


def constants(block, sizes):
    b0, b1, b2 = block
    m0, m1, m2 = (size // 2 for size in sizes)
    q0, q1, q2 = (size // 4 for size in sizes)
    c0, c1, c2 = (size // 8 for size in sizes)
    table = {}
    table["own_rows"] = np.kron(np.eye(b0 // 2), pairs(b1 // 2))
    lanes = 0.125 * pairs(b2 // 2).T
    table["own_lo"] = np.concatenate([lanes, np.zeros_like(lanes)], axis=1)
    table["own_hi"] = np.concatenate([np.zeros_like(lanes), lanes], axis=1)
    table["down_rows"] = blocked(pairs(q1))
    table["down_lanes"] = 0.125 * pairs(q2).T
    window_lanes = [b2 + j for j in range(b2 // 2)] + [j - b2 for j in range(b2 // 2, 2 * b2)]
    window_rows = [j - 8 for j in range(b1 + 16)]
    for name, weights in (("cubic", CUBIC), ("linear", LINEAR)):
        table[name + "_rows1"] = blocked(interpolation(q1, range(m1), weights))
        table[name + "_lanes1"] = interpolation(q2, range(m2), weights).T
        table[name + "_rows0"] = blocked(interpolation(m1, window_rows, weights))
        table[name + "_lanes0"] = interpolation(m2, window_lanes, weights).T
    (u0, cos0), (u1, cos1), (u2, cos2) = basis(c0), basis(c1), basis(c2)
    table["spectrum_rows"] = np.kron(u0.T @ pairs(c0), u1.T @ pairs(c1))
    table["spectrum_lanes"] = 0.125 * pairs(c2).T @ u2
    for name, weights in (("cubic", CUBIC), ("linear", LINEAR)):
        table[name + "_rows2"] = np.kron(
            interpolation(c0, range(q0), weights) @ u0, interpolation(c1, range(q1), weights) @ u1
        )
        table[name + "_lanes2"] = u2.T @ interpolation(c2, range(q2), weights).T
    two = np.float32(2.0)
    eigen = (
        np.float32(6.0)
        - two * cos0[:, None, None]
        - two * cos1[None, :, None]
        - two * cos2[None, None, :]
    )
    table["eigen"] = (np.float32(0.25 ** (LEVELS - 1)) * eigen).reshape(c0 * c1, c2)
    return {name: np.asarray(value, np.float32) for name, value in table.items()}


def dot(a, b):
    return jnp.dot(a, b, precision=PRECISE, preferred_element_type=jnp.float32)


def around(plane):
    rows, lanes = plane.shape
    total = pltpu.roll(plane, 1, 0) + pltpu.roll(plane, rows - 1, 0)
    return total + (pltpu.roll(plane, 1, 1) + pltpu.roll(plane, lanes - 1, 1))


def around_all(values):
    first = jnp.concatenate([values[1:], values[:1]], axis=0)
    first = first + jnp.concatenate([values[-1:], values[:-1]], axis=0)
    for axis in (1, 2):
        first = first + pltpu.roll(values, 1, axis)
        first = first + pltpu.roll(values, values.shape[axis] - 1, axis)
    return first


def row_blocks(matrix, values):
    depth = matrix.shape[1]
    return jnp.concatenate(
        [dot(matrix, values[i : i + depth]) for i in range(0, values.shape[0], depth)], axis=0
    )


def loop(count, body):
    def step(i, carry):
        body(i)
        return carry

    lax.fori_loop(0, count, step, 0, unroll=4 if count % 4 == 0 else 2)


def close(ref):
    count = ref.shape[0] - 2
    ref[0] = ref[count]
    ref[count + 1] = ref[1]


def defect_plane(v, p, g, weight, diagonal):
    center = v[p]
    beside = v[p - 1] + v[p + 1] + around(center)
    return center, g - (diagonal * center - weight * beside)


def restrict_own(k, summed):
    b_half, rows, lanes = summed.shape
    folded = dot(k["own_rows"][...], summed.reshape(b_half * rows, lanes))
    half = folded.shape[0] // 2
    return dot(folded[:half], k["own_lo"][...]) + dot(folded[half:], k["own_hi"][...])


def unpack(gathered, counts, g):
    nx, ny, nz = counts
    x, y, z = (lax.axis_index(name) for name in NAMES)
    half, rows, lanes = gathered.shape[1:]
    low = lax.broadcasted_iota(jnp.int32, (half, rows, lanes), 2) < lanes // 2
    for dx in range(nx):
        for dz in range(nz):
            for pair in range(ny // 2):
                parts = []
                for dy in (2 * pair, 2 * pair + 1):
                    index = (lax.rem(x + dx, nx) * ny + lax.rem(y + dy, ny)) * nz
                    parts.append(gathered[index + lax.rem(z + dz, nz)])
                turned = [pltpu.roll(part, lanes // 2, 2) for part in parts]
                where = (pl.ds(dz * rows, rows), pl.ds(pair * lanes, lanes))
                start = 2 * half * dx
                g[(pl.ds(start, half), *where)] = jnp.where(low, parts[0], turned[1])
                g[(pl.ds(start + half, half), *where)] = jnp.where(low, turned[0], parts[1])


def solve(k, kind, values, shift):
    shape = values.shape
    flat = values.reshape(shape[0] * shape[1], shape[2])
    spectrum = dot(k["spectrum_rows"][...], dot(flat, k["spectrum_lanes"][...]))
    spectrum = spectrum / (k["eigen"][...] + shift)
    fine = dot(k[kind + "_rows2"][...], dot(spectrum, k[kind + "_lanes2"][...]))
    return fine.reshape(shape)


def cycle2(k, v, g, shift):
    weight = 0.25**2
    diagonal = 6.0 * weight + shift
    damp = DAMPING / diagonal
    if v is None:
        v = damp * g
    else:
        v = v + damp * (g - (diagonal * v - weight * around_all(v)))
    v = v + solve(k, "linear", g - (diagonal * v - weight * around_all(v)), shift)
    return v + damp * (g - (diagonal * v - weight * around_all(v)))


def down(k, t, shape2):
    flat = row_blocks(k["down_rows"][...], t[...].reshape(-1, t.shape[2]))
    return dot(flat, k["down_lanes"][...]).reshape(shape2)


def up(k, kind, level, values, z):
    flat = dot(values, k[kind + "_lanes" + level][...])
    z[...] = row_blocks(k[kind + "_rows" + level][...], flat).reshape(z.shape)


def blend(z, i, weights, count):
    total = None
    for offset, weight in weights.items():
        index = i + offset
        index = index if count is None else lax.rem(index + count, count)
        term = weight * z[index]
        total = term if total is None else total + term
    return total


def up1(k, kind, values, z, v, add):
    count = z.shape[0]
    up(k, kind, "1", values.reshape(-1, values.shape[2]), z)
    weights = CUBIC if kind == "cubic" else LINEAR

    def body(i):
        for odd in (0, 1):
            p = 2 * i + odd + 1
            value = blend(z, i, weights[odd], count)
            v[p] = v[p] + value if add else value

    loop(count, body)
    close(v)


def cycle1(k, v, u, g, t, z, shift, zero, shape2):
    weight = 0.25
    diagonal = 6.0 * weight + shift
    damp = DAMPING / diagonal
    count = g.shape[0]

    def before(p):
        if zero:
            u[p + 1] = damp * g[p]
        else:
            center, rest = defect_plane(v, p + 1, g[p], weight, diagonal)
            u[p + 1] = center + damp * rest

    loop(count, before)
    close(u)

    def residue(i):
        t[i] = (
            defect_plane(u, 2 * i + 1, g[2 * i], weight, diagonal)[1]
            + defect_plane(u, 2 * i + 2, g[2 * i + 1], weight, diagonal)[1]
        )

    loop(count // 2, residue)
    correction = cycle2(k, None, down(k, t, shape2), shift)
    up1(k, "linear", correction, z, u, True)

    def after(p):
        center, rest = defect_plane(u, p + 1, g[p], weight, diagonal)
        v[p + 1] = center + damp * rest

    loop(count, after)
    close(v)


def window(k, kind, v, zw, span, write):
    count = v.shape[0] - 2
    values = jnp.concatenate([v[count - 3 : count + 1], v[1 : span - 3]], axis=0)
    up(k, kind, "0", values.reshape(-1, values.shape[2]), zw)
    weights = CUBIC if kind == "cubic" else LINEAR

    def body(i):
        for odd in (0, 1):
            write(2 * i + odd, blend(zw, i + 3, weights[odd], None))

    loop(span - 6, body)


def own_defect(v, p, f, weight, diagonal):
    rows, lanes = f.shape
    inside = (pl.ds(8, rows), pl.ds(lanes, lanes))
    wide = v[p + 1, pl.ds(8, rows), :]
    center = wide[:, lanes:]
    beside = v[(p, *inside)] + v[(p + 2, *inside)]
    beside = beside + v[p + 1, pl.ds(7, rows), pl.ds(lanes, lanes)]
    beside = beside + v[p + 1, pl.ds(9, rows), pl.ds(lanes, lanes)]
    beside = beside + pltpu.roll(wide, 1, 1)[:, lanes:]
    beside = beside + pltpu.roll(wide, 2 * lanes - 1, 1)[:, lanes:]
    return center, f - (diagonal * center - weight * beside)


def first_kernel(names, *refs):
    k = dict(zip(names, refs))
    source, out = refs[len(names) :]
    b0, b1, b2 = source.shape
    summed = source[...].reshape(b0 // 2, 2, b1, b2)
    out[...] = restrict_own(k, summed[:, 0] + summed[:, 1]).reshape(out.shape)


def second_kernel(names, counts, shape2, span, *refs):
    k = dict(zip(names, refs))
    (shift_ref, gathered, source, plane_lo, plane_hi, row_lo, row_hi, lane_halo) = refs[
        len(names) : len(names) + 8
    ]
    out, v1, g, v, u, t, z, zw, v0, f, summed = refs[len(names) + 8 :]
    shift = shift_ref[0]
    unpack(gathered, counts, g)
    b0, b1, b2 = source.shape
    f[...] = jnp.zeros_like(f)
    rows, lanes = pl.ds(8, b1), pl.ds(b2, b2)
    f[1 : b0 + 1, rows, lanes] = source[...]
    f[0, rows, lanes] = plane_lo[0]
    f[b0 + 1, rows, lanes] = plane_hi[0]
    f[1 : b0 + 1, pl.ds(7, 1), lanes] = row_lo[...]
    f[1 : b0 + 1, pl.ds(8 + b1, 1), lanes] = row_hi[...]
    f[1 : b0 + 1, rows, pl.ds(0, b2)] = lane_halo[...]
    def pair_sum(i):
        t[i] = g[2 * i] + g[2 * i + 1]

    loop(g.shape[0] // 2, pair_sum)
    forcing2 = down(k, t, shape2)
    iterate2 = cycle2(k, solve(k, "cubic", forcing2, shift), forcing2, shift)
    up1(k, "cubic", iterate2, z, v, False)
    cycle1(k, v, u, g, t, z, shift, False, shape2)

    def put(p, value):
        v0[p] = value

    window(k, "cubic", v, zw, span, put)
    diagonal = 6.0 + shift
    damp = DAMPING / diagonal

    def before(p):
        center, rest = defect_plane(v0, p + 1, f[p], 1.0, diagonal)
        v1[p] = center + damp * rest

    loop(b0 + 2, before)

    def residue(i):
        summed[i] = (
            own_defect(v1, 2 * i, source[2 * i], 1.0, diagonal)[1]
            + own_defect(v1, 2 * i + 1, source[2 * i + 1], 1.0, diagonal)[1]
        )

    loop(b0 // 2, residue)
    out[...] = restrict_own(k, summed[...]).reshape(out.shape)


def third_kernel(names, counts, shape2, span, *refs):
    k = dict(zip(names, refs))
    shift_ref, gathered, source, v1, out, g, v, u, t, z, zw, w = refs[len(names) :]
    shift = shift_ref[0]
    unpack(gathered, counts, g)
    cycle1(k, v, u, g, t, z, shift, True, shape2)
    b0 = source.shape[0]

    def put(p, value):
        w[p] = value

    window(k, "linear", v, zw, span, put)

    def add(p):
        w[p] = v1[p] + w[p + 1]

    loop(b0 + 2, add)
    diagonal = 6.0 + shift
    damp = DAMPING / diagonal

    def after(p):
        center, rest = own_defect(w, p, source[p], 1.0, diagonal)
        out[p] = center + damp * rest

    loop(b0, after)


def beside(values, axis, step):
    count = lax.axis_size(axis)
    return lax.ppermute(values, axis, [(i, (i + step) % count) for i in range(count)])


def per_device(counts, source, shift):
    nx, ny, nz = counts
    b0, b1, b2 = source.shape
    sizes = (b0 * nx, b1 * nz, b2 * ny)
    table = constants(source.shape, sizes)
    m0, m1, m2 = (size // 2 for size in sizes)
    shape2 = tuple(size // 4 for size in sizes)
    span = b0 // 2 + 8
    wide = (b1 + 16, 2 * b2)
    packed = jax.ShapeDtypeStruct((b0 // 4, b1 // 2, b2), jnp.float32)
    vmem = pl.BlockSpec(memory_space=pltpu.VMEM)
    params = pltpu.CompilerParams(vmem_limit_bytes=60 * 1024 * 1024)

    def field(*shape):
        return pltpu.VMEM(shape, jnp.float32)

    def run(body, names, operands, outs, scratch, smem):
        specs = [vmem] * len(names)
        specs += [pl.BlockSpec(memory_space=pltpu.SMEM)] * smem
        specs += [vmem] * (len(operands) - smem)
        return pl.pallas_call(
            functools.partial(body, names),
            out_shape=outs,
            in_specs=specs,
            out_specs=[vmem] * len(outs) if isinstance(outs, tuple) else vmem,
            scratch_shapes=scratch,
            compiler_params=params,
        )(*[jnp.asarray(table[name]) for name in names], *operands)

    own = ("own_rows", "own_lo", "own_hi")
    coarse = ("down_rows", "down_lanes", "spectrum_rows", "spectrum_lanes", "eigen")
    linear = tuple(name for name in table if name.startswith("linear"))
    linear_low = tuple(name for name in linear if not name.endswith("0"))
    cubic = tuple(name for name in table if name.startswith("cubic"))
    plane_lo = beside(source[-1:], "gx", 1)
    plane_hi = beside(source[:1], "gx", -1)
    row_lo = beside(source[:, -1:], "gz", 1)
    row_hi = beside(source[:, :1], "gz", -1)
    lane_lo = beside(source[:, :, -1], "gy", 1)
    lane_hi = beside(source[:, :, 0], "gy", -1)
    lane_halo = jnp.concatenate(
        [lane_hi[:, :, None], jnp.zeros((b0, b1, b2 - 2), jnp.float32), lane_lo[:, :, None]], axis=2
    )
    buffers = [
        field(m0, m1, m2),
        field(m0 + 2, m1, m2),
        field(m0 + 2, m1, m2),
        field(m0 // 2, m1, m2),
        field(m0 // 2, m1, m2),
        field(span, *wide),
    ]
    block = run(first_kernel, own, (source,), packed, [], 0)
    gathered = lax.all_gather(block, NAMES, axis=0)
    block, v1 = run(
        lambda names, *refs: second_kernel(names, counts, shape2, span, *refs),
        own + coarse + linear_low + cubic,
        (shift, gathered, source, plane_lo, plane_hi, row_lo, row_hi, lane_halo),
        (packed, jax.ShapeDtypeStruct((b0 + 2, *wide), jnp.float32)),
        buffers + [field(b0 + 4, *wide), field(b0 + 2, *wide), field(b0 // 2, b1, b2)],
        1,
    )
    gathered = lax.all_gather(block, NAMES, axis=0)
    return run(
        lambda names, *refs: third_kernel(names, counts, shape2, span, *refs),
        coarse + linear,
        (shift, gathered, source, v1),
        jax.ShapeDtypeStruct(source.shape, jnp.float32),
        buffers + [field(b0 + 4, *wide)],
        1,
    )


def solution(mesh):
    counts = tuple(mesh.shape[name] for name in NAMES)
    return jax.shard_map(
        functools.partial(per_device, counts),
        mesh=mesh,
        in_specs=(P("gx", "gz", "gy"), P()),
        out_specs=P("gx", "gz", "gy"),
        check_vma=False,
    )
```

```python
import functools

import jax
import jax.numpy as jnp
import numpy as np
from jax import lax
from jax.experimental import pallas as pl
from jax.experimental.pallas import tpu as pltpu
from jax.sharding import PartitionSpec as P

LEVELS = 4
DAMPING = 6.0 / 7.0
PRECISE = lax.Precision.HIGHEST
CUBIC = (
    {-2: -5.0 / 128.0, -1: 35.0 / 128.0, 0: 105.0 / 128.0, 1: -7.0 / 128.0},
    {-1: -7.0 / 128.0, 0: 105.0 / 128.0, 1: 35.0 / 128.0, 2: -5.0 / 128.0},
)
LINEAR = ({-1: 0.25, 0: 0.75}, {0: 0.75, 1: 0.25})
NAMES = ("gx", "gy", "gz")
MESH = pl.DeviceIdType.MESH


def basis(count):
    cells = np.arange(count)
    columns, cosines = [], []
    for m in range(count):
        k = (m + 1) // 2
        angle = 2.0 * np.pi * k * cells / count
        column = np.cos(angle) if m % 2 == 1 or m == 0 else np.sin(angle)
        columns.append(column / np.sqrt(np.sum(column**2)))
        cosines.append(np.cos(2.0 * np.pi * k / count))
    return np.stack(columns, axis=1), np.array(cosines, np.float32)


def interpolation(coarse_count, fine_cells, weights):
    matrix = np.zeros((len(fine_cells), coarse_count))
    for row, cell in enumerate(fine_cells):
        for offset, weight in weights[cell % 2].items():
            matrix[row, (cell // 2 + offset) % coarse_count] += weight
    return matrix


def pairs(coarse_count):
    return np.kron(np.eye(coarse_count), np.ones((1, 2)))


def blocked(matrix):
    count = max(1, 128 // matrix.shape[1])
    return np.kron(np.eye(count), matrix)


def constants(block, sizes):
    b0, b1, b2 = block
    m0, m1, m2 = (size // 2 for size in sizes)
    q0, q1, q2 = (size // 4 for size in sizes)
    c0, c1, c2 = (size // 8 for size in sizes)
    table = {}
    table["own_rows"] = np.kron(np.eye(b0 // 2), pairs(b1 // 2))
    lanes = 0.125 * pairs(b2 // 2).T
    table["own_lo"] = np.concatenate([lanes, np.zeros_like(lanes)], axis=1)
    table["own_hi"] = np.concatenate([np.zeros_like(lanes), lanes], axis=1)
    table["down_rows"] = blocked(pairs(q1))
    table["down_lanes"] = 0.125 * pairs(q2).T
    window_lanes = [b2 + j for j in range(b2 // 2)] + [j - b2 for j in range(b2 // 2, 2 * b2)]
    window_rows = [j - 8 for j in range(b1 + 16)]
    for name, weights in (("cubic", CUBIC), ("linear", LINEAR)):
        table[name + "_rows1"] = blocked(interpolation(q1, range(m1), weights))
        table[name + "_lanes1"] = interpolation(q2, range(m2), weights).T
        table[name + "_rows0"] = blocked(interpolation(m1, window_rows, weights))
        table[name + "_lanes0"] = interpolation(m2, window_lanes, weights).T
    (u0, cos0), (u1, cos1), (u2, cos2) = basis(c0), basis(c1), basis(c2)
    table["spectrum_rows"] = np.kron(u0.T @ pairs(c0), u1.T @ pairs(c1))
    table["spectrum_lanes"] = 0.125 * pairs(c2).T @ u2
    for name, weights in (("cubic", CUBIC), ("linear", LINEAR)):
        table[name + "_rows2"] = np.kron(
            interpolation(c0, range(q0), weights) @ u0, interpolation(c1, range(q1), weights) @ u1
        )
        table[name + "_lanes2"] = u2.T @ interpolation(c2, range(q2), weights).T
    two = np.float32(2.0)
    eigen = (
        np.float32(6.0)
        - two * cos0[:, None, None]
        - two * cos1[None, :, None]
        - two * cos2[None, None, :]
    )
    table["eigen"] = (np.float32(0.25 ** (LEVELS - 1)) * eigen).reshape(c0 * c1, c2)
    return {name: np.asarray(value, np.float32) for name, value in table.items()}


def dot(a, b):
    return jnp.dot(a, b, precision=PRECISE, preferred_element_type=jnp.float32)


def around(plane):
    rows, lanes = plane.shape
    total = pltpu.roll(plane, 1, 0) + pltpu.roll(plane, rows - 1, 0)
    return total + (pltpu.roll(plane, 1, 1) + pltpu.roll(plane, lanes - 1, 1))


def around_all(values):
    first = jnp.concatenate([values[1:], values[:1]], axis=0)
    first = first + jnp.concatenate([values[-1:], values[:-1]], axis=0)
    for axis in (1, 2):
        first = first + pltpu.roll(values, 1, axis)
        first = first + pltpu.roll(values, values.shape[axis] - 1, axis)
    return first


def row_blocks(matrix, values):
    depth = matrix.shape[1]
    return jnp.concatenate(
        [dot(matrix, values[i : i + depth]) for i in range(0, values.shape[0], depth)], axis=0
    )


def loop(count, body):
    def step(i, carry):
        body(i)
        return carry

    lax.fori_loop(0, count, step, 0, unroll=4 if count % 4 == 0 else 2)


def close(ref):
    count = ref.shape[0] - 2
    ref[0] = ref[count]
    ref[count + 1] = ref[1]


def defect_plane(v, p, g, weight, diagonal):
    center = v[p]
    beside = v[p - 1] + v[p + 1] + around(center)
    return center, g - (diagonal * center - weight * beside)


def restrict_own(k, summed):
    b_half, rows, lanes = summed.shape
    folded = dot(k["own_rows"][...], summed.reshape(b_half * rows, lanes))
    half = folded.shape[0] // 2
    return dot(folded[:half], k["own_lo"][...]) + dot(folded[half:], k["own_hi"][...])


def unpack(gathered, counts, g):
    nx, ny, nz = counts
    x, y, z = (lax.axis_index(name) for name in NAMES)
    half, rows, lanes = gathered.shape[1:]
    low = lax.broadcasted_iota(jnp.int32, (half, rows, lanes), 2) < lanes // 2
    for dx in range(nx):
        for dz in range(nz):
            for pair in range(ny // 2):
                parts = []
                for dy in (2 * pair, 2 * pair + 1):
                    index = (lax.rem(x + dx, nx) * ny + lax.rem(y + dy, ny)) * nz
                    parts.append(gathered[index + lax.rem(z + dz, nz)])
                turned = [pltpu.roll(part, lanes // 2, 2) for part in parts]
                where = (pl.ds(dz * rows, rows), pl.ds(pair * lanes, lanes))
                start = 2 * half * dx
                g[(pl.ds(start, half), *where)] = jnp.where(low, parts[0], turned[1])
                g[(pl.ds(start + half, half), *where)] = jnp.where(low, turned[0], parts[1])


def solve(k, kind, values, shift):
    shape = values.shape
    flat = values.reshape(shape[0] * shape[1], shape[2])
    spectrum = dot(k["spectrum_rows"][...], dot(flat, k["spectrum_lanes"][...]))
    spectrum = spectrum / (k["eigen"][...] + shift)
    fine = dot(k[kind + "_rows2"][...], dot(spectrum, k[kind + "_lanes2"][...]))
    return fine.reshape(shape)


def cycle2(k, v, g, shift):
    weight = 0.25**2
    diagonal = 6.0 * weight + shift
    damp = DAMPING / diagonal
    if v is None:
        v = damp * g
    else:
        v = v + damp * (g - (diagonal * v - weight * around_all(v)))
    v = v + solve(k, "linear", g - (diagonal * v - weight * around_all(v)), shift)
    return v + damp * (g - (diagonal * v - weight * around_all(v)))


def down(k, t, shape2):
    flat = row_blocks(k["down_rows"][...], t[...].reshape(-1, t.shape[2]))
    return dot(flat, k["down_lanes"][...]).reshape(shape2)


def up(k, kind, level, values, z):
    flat = dot(values, k[kind + "_lanes" + level][...])
    z[...] = row_blocks(k[kind + "_rows" + level][...], flat).reshape(z.shape)


def blend(z, i, weights, count):
    total = None
    for offset, weight in weights.items():
        index = i + offset
        index = index if count is None else lax.rem(index + count, count)
        term = weight * z[index]
        total = term if total is None else total + term
    return total


def up1(k, kind, values, z, v, add):
    count = z.shape[0]
    up(k, kind, "1", values.reshape(-1, values.shape[2]), z)
    weights = CUBIC if kind == "cubic" else LINEAR

    def body(i):
        for odd in (0, 1):
            p = 2 * i + odd + 1
            value = blend(z, i, weights[odd], count)
            v[p] = v[p] + value if add else value

    loop(count, body)
    close(v)


def cycle1(k, v, u, g, t, z, shift, zero, shape2):
    weight = 0.25
    diagonal = 6.0 * weight + shift
    damp = DAMPING / diagonal
    count = g.shape[0]

    def before(p):
        if zero:
            u[p + 1] = damp * g[p]
        else:
            center, rest = defect_plane(v, p + 1, g[p], weight, diagonal)
            u[p + 1] = center + damp * rest

    loop(count, before)
    close(u)

    def residue(i):
        t[i] = (
            defect_plane(u, 2 * i + 1, g[2 * i], weight, diagonal)[1]
            + defect_plane(u, 2 * i + 2, g[2 * i + 1], weight, diagonal)[1]
        )

    loop(count // 2, residue)
    correction = cycle2(k, None, down(k, t, shape2), shift)
    up1(k, "linear", correction, z, u, True)

    def after(p):
        center, rest = defect_plane(u, p + 1, g[p], weight, diagonal)
        v[p + 1] = center + damp * rest

    loop(count, after)
    close(v)


def window(k, kind, v, zw, span, write):
    count = v.shape[0] - 2
    values = jnp.concatenate([v[count - 3 : count + 1], v[1 : span - 3]], axis=0)
    up(k, kind, "0", values.reshape(-1, values.shape[2]), zw)
    weights = CUBIC if kind == "cubic" else LINEAR

    def body(i):
        for odd in (0, 1):
            write(2 * i + odd, blend(zw, i + 3, weights[odd], None))

    loop(span - 6, body)


def own_defect(v, p, f, weight, diagonal):
    rows, lanes = f.shape
    inside = (pl.ds(8, rows), pl.ds(lanes, lanes))
    wide = v[p + 1, pl.ds(8, rows), :]
    center = wide[:, lanes:]
    beside = v[(p, *inside)] + v[(p + 2, *inside)]
    beside = beside + v[p + 1, pl.ds(7, rows), pl.ds(lanes, lanes)]
    beside = beside + v[p + 1, pl.ds(9, rows), pl.ds(lanes, lanes)]
    beside = beside + pltpu.roll(wide, 1, 1)[:, lanes:]
    beside = beside + pltpu.roll(wide, 2 * lanes - 1, 1)[:, lanes:]
    return center, f - (diagonal * center - weight * beside)


def position():
    return tuple(lax.axis_index(name) for name in NAMES)


def partner_of(place):
    x, y, z = place
    return (x, y + 1 - 2 * lax.rem(y, 2), z)


def shifted(place, counts, offset):
    return tuple(
        lax.rem(at + step + count, count) for at, step, count in zip(place, offset, counts)
    )


def slot(place, counts):
    return (place[0] * counts[1] + place[1]) * counts[2] + place[2]


def chip_offsets(counts):
    nx, ny, nz = counts
    offsets = [
        (dx, dy, dz) for dx in range(nx) for dy in range(0, ny, 2) for dz in range(nz)
    ]

    def hops(offset):
        return sum(min(step, count - step) for step, count in zip(offset, (nx, ny, nz)))

    return sorted(offsets[1:], key=hops, reverse=True)


def face_offsets(counts):
    faces = []
    for axis in range(3):
        for side, step in ((0, -1), (1, 1)):
            offset = [0, 0, 0]
            offset[axis] = step
            faces.append((tuple(offset), axis, side))
    return faces


def greet(barrier, places):
    for place in places:
        pl.semaphore_signal(barrier, inc=1, device_id=place, device_id_type=MESH)


def remote(src, dst, send, recv, place):
    return pltpu.make_async_remote_copy(
        src_ref=src, dst_ref=dst, send_sem=send, recv_sem=recv, device_id=place, device_id_type=MESH
    )


def spread(counts, block, gathered, sems):
    send, recv, relay_send, relay_recv = sems
    me = position()
    partner = partner_of(me)
    offsets = chip_offsets(counts)
    mine = gathered.at[slot(me, counts)]
    copies = []
    for n, offset in enumerate(offsets):
        place = shifted(me, counts, offset)
        copies.append(remote(block, mine, send.at[n], recv.at[n], place))
        copies[-1].start()
    last = len(offsets)
    relays = [remote(block, mine, relay_send.at[last], relay_recv.at[last], partner)]
    relays[0].start()

    def finish():
        gathered[slot(me, counts)] = block[...]
        for n, offset in reversed(list(enumerate(offsets))):
            copies[n].wait_recv()
            source = shifted(me, counts, tuple(-step for step in offset))
            arrived = gathered.at[slot(source, counts)]
            relays.append(
                remote(arrived, arrived, relay_send.at[n], relay_recv.at[n], partner)
            )
            relays[-1].start()
        for copy in copies:
            copy.wait_send()
        for relay in relays:
            relay.wait()

    return finish


def gather_places(counts):
    me = position()
    return [shifted(me, counts, offset) for offset in chip_offsets(counts)] + [partner_of(me)]


def first_kernel(names, counts, *refs):
    k = dict(zip(names, refs))
    (source, gathered, planes, rows, columns) = refs[len(names) : len(names) + 5]
    block, own_planes, own_rows, own_columns, *sems, face_send, face_recv = refs[len(names) + 5 :]
    me = position()
    barrier = pltpu.get_barrier_semaphore()
    faces = face_offsets(counts)
    places = gather_places(counts) + [shifted(me, counts, offset) for offset, _, _ in faces]
    greet(barrier, places)
    b0, b1, b2 = source.shape
    summed = source[...].reshape(b0 // 2, 2, b1, b2)
    block[...] = restrict_own(k, summed[:, 0] + summed[:, 1]).reshape(block.shape)
    own_planes[0] = source[0]
    own_planes[1] = source[b0 - 1]
    own_rows[0] = source[:, pl.ds(0, 1), :]
    own_rows[1] = source[:, pl.ds(b1 - 1, 1), :]
    turned = source[...].reshape(b0 * b1, b2).T
    own_columns[0] = turned[:8]
    own_columns[1] = turned[b2 - 8 :]
    pl.semaphore_wait(barrier, len(places))
    finish = spread(counts, block, gathered, sems)
    buffers = ((own_planes, planes), (own_rows, rows), (own_columns, columns))
    order = (0, 2, 1)
    copies = []
    for n, (offset, axis, side) in enumerate(faces):
        own, halo = buffers[order[axis]]
        place = shifted(me, counts, offset)
        copies.append(
            remote(own.at[side], halo.at[1 - side], face_send.at[n], face_recv.at[n], place)
        )
        copies[-1].start()
    finish()
    for copy in copies:
        copy.wait()


def gather_kernel(counts, block, gathered, *sems):
    barrier = pltpu.get_barrier_semaphore()
    places = gather_places(counts)
    greet(barrier, places)
    pl.semaphore_wait(barrier, len(places))
    spread(counts, block, gathered, sems)()


def second_kernel(names, counts, shape2, span, *refs):
    k = dict(zip(names, refs))
    (shift_ref, gathered, source, plane_halo, row_halo, column_halo) = refs[
        len(names) : len(names) + 6
    ]
    out, v1, g, v, u, t, z, zw, v0, f, summed = refs[len(names) + 6 :]
    shift = shift_ref[0]
    unpack(gathered, counts, g)
    b0, b1, b2 = source.shape
    f[...] = jnp.zeros_like(f)
    rows, lanes = pl.ds(8, b1), pl.ds(b2, b2)
    f[1 : b0 + 1, rows, lanes] = source[...]
    f[0, rows, lanes] = plane_halo[0]
    f[b0 + 1, rows, lanes] = plane_halo[1]
    f[1 : b0 + 1, pl.ds(7, 1), lanes] = row_halo[0]
    f[1 : b0 + 1, pl.ds(8 + b1, 1), lanes] = row_halo[1]
    middle = jnp.zeros((b2 - 16, b0 * b1), jnp.float32)
    turned = jnp.concatenate([column_halo[1], middle, column_halo[0]], axis=0)
    f[1 : b0 + 1, rows, pl.ds(0, b2)] = turned.T.reshape(b0, b1, b2)
    def pair_sum(i):
        t[i] = g[2 * i] + g[2 * i + 1]

    loop(g.shape[0] // 2, pair_sum)
    forcing2 = down(k, t, shape2)
    iterate2 = cycle2(k, solve(k, "cubic", forcing2, shift), forcing2, shift)
    up1(k, "cubic", iterate2, z, v, False)
    cycle1(k, v, u, g, t, z, shift, False, shape2)

    def put(p, value):
        v0[p] = value

    window(k, "cubic", v, zw, span, put)
    diagonal = 6.0 + shift
    damp = DAMPING / diagonal

    def before(p):
        center, rest = defect_plane(v0, p + 1, f[p], 1.0, diagonal)
        v1[p] = center + damp * rest

    loop(b0 + 2, before)

    def residue(i):
        summed[i] = (
            own_defect(v1, 2 * i, source[2 * i], 1.0, diagonal)[1]
            + own_defect(v1, 2 * i + 1, source[2 * i + 1], 1.0, diagonal)[1]
        )

    loop(b0 // 2, residue)
    out[...] = restrict_own(k, summed[...]).reshape(out.shape)


def third_kernel(names, counts, shape2, span, *refs):
    k = dict(zip(names, refs))
    shift_ref, gathered, source, v1, out, g, v, u, t, z, zw, w = refs[len(names) :]
    shift = shift_ref[0]
    unpack(gathered, counts, g)
    cycle1(k, v, u, g, t, z, shift, True, shape2)
    b0 = source.shape[0]

    def put(p, value):
        w[p] = value

    window(k, "linear", v, zw, span, put)

    def add(p):
        w[p] = v1[p] + w[p + 1]

    loop(b0 + 2, add)
    diagonal = 6.0 + shift
    damp = DAMPING / diagonal

    def after(p):
        center, rest = own_defect(w, p, source[p], 1.0, diagonal)
        out[p] = center + damp * rest

    loop(b0, after)


def per_device(counts, source, shift):
    nx, ny, nz = counts
    b0, b1, b2 = source.shape
    sizes = (b0 * nx, b1 * nz, b2 * ny)
    table = constants(source.shape, sizes)
    m0, m1, m2 = (size // 2 for size in sizes)
    shape2 = tuple(size // 4 for size in sizes)
    span = b0 // 2 + 8
    wide = (b1 + 16, 2 * b2)
    packed = jax.ShapeDtypeStruct((b0 // 4, b1 // 2, b2), jnp.float32)
    vmem = pl.BlockSpec(memory_space=pltpu.VMEM)

    def field(*shape):
        return pltpu.VMEM(shape, jnp.float32)

    def run(body, names, operands, outs, scratch, smem, collective=None):
        specs = [vmem] * len(names)
        specs += [pl.BlockSpec(memory_space=pltpu.SMEM)] * smem
        specs += [vmem] * (len(operands) - smem)
        return pl.pallas_call(
            functools.partial(body, names),
            out_shape=outs,
            in_specs=specs,
            out_specs=[vmem] * len(outs) if isinstance(outs, tuple) else vmem,
            scratch_shapes=scratch,
            compiler_params=pltpu.CompilerParams(
                vmem_limit_bytes=60 * 1024 * 1024,
                collective_id=collective,
                has_side_effects=collective is not None,
            ),
        )(*[jnp.asarray(table[name]) for name in names], *operands)

    own = ("own_rows", "own_lo", "own_hi")
    coarse = ("down_rows", "down_lanes", "spectrum_rows", "spectrum_lanes", "eigen")
    linear = tuple(name for name in table if name.startswith("linear"))
    linear_low = tuple(name for name in linear if not name.endswith("0"))
    cubic = tuple(name for name in table if name.startswith("cubic"))
    buffers = [
        field(m0, m1, m2),
        field(m0 + 2, m1, m2),
        field(m0 + 2, m1, m2),
        field(m0 // 2, m1, m2),
        field(m0 // 2, m1, m2),
        field(span, *wide),
    ]
    devices = nx * ny * nz
    chips = devices // 2
    sems = [pltpu.SemaphoreType.DMA((max(chips - 1, 1),))] * 2
    sems += [pltpu.SemaphoreType.DMA((chips,))] * 2
    everyone = jax.ShapeDtypeStruct((devices, *packed.shape), jnp.float32)
    face_shapes = ((2, b1, b2), (2, b0, 1, b2), (2, 8, b0 * b1))
    gathered, *halos = run(
        lambda names, *refs: first_kernel(names, counts, *refs),
        own,
        (source,),
        (everyone, *[jax.ShapeDtypeStruct(shape, jnp.float32) for shape in face_shapes]),
        [field(*packed.shape), *[field(*shape) for shape in face_shapes], *sems]
        + [pltpu.SemaphoreType.DMA((6,))] * 2,
        0,
        0,
    )
    block, v1 = run(
        lambda names, *refs: second_kernel(names, counts, shape2, span, *refs),
        own + coarse + linear_low + cubic,
        (shift, gathered, source, *halos),
        (packed, jax.ShapeDtypeStruct((b0 + 2, *wide), jnp.float32)),
        buffers + [field(b0 + 4, *wide), field(b0 + 2, *wide), field(b0 // 2, b1, b2)],
        1,
    )
    gathered = run(
        lambda names, *refs: gather_kernel(counts, *refs), (), (block,), everyone, sems, 0, 1
    )
    return run(
        lambda names, *refs: third_kernel(names, counts, shape2, span, *refs),
        coarse + linear,
        (shift, gathered, source, v1),
        jax.ShapeDtypeStruct(source.shape, jnp.float32),
        buffers + [field(b0 + 4, *wide)],
        1,
    )


def solution(mesh):
    counts = tuple(mesh.shape[name] for name in NAMES)
    return jax.shard_map(
        functools.partial(per_device, counts),
        mesh=mesh,
        in_specs=(P("gx", "gz", "gy"), P()),
        out_specs=P("gx", "gz", "gy"),
        check_vma=False,
    )
```

```python
import functools

import jax
import jax.numpy as jnp
import numpy as np
from jax import lax
from jax.experimental import pallas as pl
from jax.experimental.pallas import tpu as pltpu
from jax.sharding import PartitionSpec as P

LEVELS = 4
DAMPING = 6.0 / 7.0
PRECISE = lax.Precision.HIGHEST
CUBIC = (
    {-2: -5.0 / 128.0, -1: 35.0 / 128.0, 0: 105.0 / 128.0, 1: -7.0 / 128.0},
    {-1: -7.0 / 128.0, 0: 105.0 / 128.0, 1: 35.0 / 128.0, 2: -5.0 / 128.0},
)
LINEAR = ({-1: 0.25, 0: 0.75}, {0: 0.75, 1: 0.25})
NAMES = ("gx", "gy", "gz")
MESH = pl.DeviceIdType.MESH


def basis(count):
    cells = np.arange(count)
    columns, cosines = [], []
    for m in range(count):
        k = (m + 1) // 2
        angle = 2.0 * np.pi * k * cells / count
        column = np.cos(angle) if m % 2 == 1 or m == 0 else np.sin(angle)
        columns.append(column / np.sqrt(np.sum(column**2)))
        cosines.append(np.cos(2.0 * np.pi * k / count))
    return np.stack(columns, axis=1), np.array(cosines, np.float32)


def interpolation(coarse_count, fine_cells, weights):
    matrix = np.zeros((len(fine_cells), coarse_count))
    for row, cell in enumerate(fine_cells):
        for offset, weight in weights[cell % 2].items():
            matrix[row, (cell // 2 + offset) % coarse_count] += weight
    return matrix


def pairs(coarse_count):
    return np.kron(np.eye(coarse_count), np.ones((1, 2)))


def blocked(matrix):
    count = max(1, 128 // matrix.shape[1])
    return np.kron(np.eye(count), matrix)


def constants(block, sizes):
    b0, b1, b2 = block
    m0, m1, m2 = (size // 2 for size in sizes)
    q0, q1, q2 = (size // 4 for size in sizes)
    c0, c1, c2 = (size // 8 for size in sizes)
    table = {}
    table["own_rows"] = np.kron(np.eye(b0 // 2), pairs(b1 // 2))
    lanes = 0.125 * pairs(b2 // 2).T
    table["own_lo"] = np.concatenate([lanes, np.zeros_like(lanes)], axis=1)
    table["own_hi"] = np.concatenate([np.zeros_like(lanes), lanes], axis=1)
    table["down_rows"] = blocked(pairs(q1))
    table["down_lanes"] = 0.125 * pairs(q2).T
    window_lanes = [b2 + j for j in range(b2 // 2)] + [j - b2 for j in range(b2 // 2, 2 * b2)]
    window_rows = [j - 8 for j in range(b1 + 16)]
    for name, weights in (("cubic", CUBIC), ("linear", LINEAR)):
        table[name + "_rows1"] = blocked(interpolation(q1, range(m1), weights))
        table[name + "_lanes1"] = interpolation(q2, range(m2), weights).T
        table[name + "_rows0"] = blocked(interpolation(m1, window_rows, weights))
        table[name + "_lanes0"] = interpolation(m2, window_lanes, weights).T
    (u0, cos0), (u1, cos1), (u2, cos2) = basis(c0), basis(c1), basis(c2)
    table["spectrum_rows"] = np.kron(u0.T @ pairs(c0), u1.T @ pairs(c1))
    table["spectrum_lanes"] = 0.125 * pairs(c2).T @ u2
    for name, weights in (("cubic", CUBIC), ("linear", LINEAR)):
        table[name + "_rows2"] = np.kron(
            interpolation(c0, range(q0), weights) @ u0, interpolation(c1, range(q1), weights) @ u1
        )
        table[name + "_lanes2"] = u2.T @ interpolation(c2, range(q2), weights).T
    two = np.float32(2.0)
    eigen = (
        np.float32(6.0)
        - two * cos0[:, None, None]
        - two * cos1[None, :, None]
        - two * cos2[None, None, :]
    )
    table["eigen"] = (np.float32(0.25 ** (LEVELS - 1)) * eigen).reshape(c0 * c1, c2)
    wide = ("spectrum_rows", "spectrum_lanes", "eigen")
    return {
        name: np.asarray(
            value, np.float32 if name in wide or name.endswith("2") else jnp.bfloat16
        )
        for name, value in table.items()
    }


def dot(a, b):
    return jnp.dot(a, b, precision=PRECISE, preferred_element_type=jnp.float32)


def parts_of(values, pieces):
    parts = []
    for n in range(pieces):
        parts.append(values.astype(jnp.bfloat16))
        if n + 1 < pieces:
            values = values - parts[-1].astype(jnp.float32)
    return parts[::-1]


def right(values, matrix, pieces):
    terms = [
        jnp.dot(part, matrix, preferred_element_type=jnp.float32)
        for part in parts_of(values, pieces)
    ]
    return sum(terms[1:], terms[0])


def left(matrix, values, pieces):
    terms = [
        jnp.dot(matrix, part, preferred_element_type=jnp.float32)
        for part in parts_of(values, pieces)
    ]
    return sum(terms[1:], terms[0])


def around(plane):
    rows, lanes = plane.shape
    total = pltpu.roll(plane, 1, 0) + pltpu.roll(plane, rows - 1, 0)
    return total + (pltpu.roll(plane, 1, 1) + pltpu.roll(plane, lanes - 1, 1))


def around_all(values):
    first = jnp.concatenate([values[1:], values[:1]], axis=0)
    first = first + jnp.concatenate([values[-1:], values[:-1]], axis=0)
    for axis in (1, 2):
        first = first + pltpu.roll(values, 1, axis)
        first = first + pltpu.roll(values, values.shape[axis] - 1, axis)
    return first


def row_blocks(matrix, values, pieces):
    depth = matrix.shape[1]
    return jnp.concatenate(
        [left(matrix, values[i : i + depth], pieces) for i in range(0, values.shape[0], depth)], axis=0
    )


def loop(count, body):
    def step(i, carry):
        body(i)
        return carry

    lax.fori_loop(0, count, step, 0, unroll=4 if count % 4 == 0 else 2)


def close(ref):
    count = ref.shape[0] - 2
    ref[0] = ref[count]
    ref[count + 1] = ref[1]


def defect_plane(v, p, g, weight, diagonal):
    center = v[p]
    beside = v[p - 1] + v[p + 1] + around(center)
    return center, g - (diagonal * center - weight * beside)


def restrict_own(k, summed):
    b_half, rows, lanes = summed.shape
    folded = left(k["own_rows"][...], summed.reshape(b_half * rows, lanes), 3)
    half = folded.shape[0] // 2
    return right(folded[:half], k["own_lo"][...], 3) + right(folded[half:], k["own_hi"][...], 3)


def unpack(gathered, counts, g):
    nx, ny, nz = counts
    x, y, z = (lax.axis_index(name) for name in NAMES)
    half, rows, lanes = gathered.shape[1:]
    low = lax.broadcasted_iota(jnp.int32, (half, rows, lanes), 2) < lanes // 2
    for dx in range(nx):
        for dz in range(nz):
            for pair in range(ny // 2):
                parts = []
                for dy in (2 * pair, 2 * pair + 1):
                    index = (lax.rem(x + dx, nx) * ny + lax.rem(y + dy, ny)) * nz
                    parts.append(gathered[index + lax.rem(z + dz, nz)])
                turned = [pltpu.roll(part, lanes // 2, 2) for part in parts]
                where = (pl.ds(dz * rows, rows), pl.ds(pair * lanes, lanes))
                start = 2 * half * dx
                g[(pl.ds(start, half), *where)] = jnp.where(low, parts[0], turned[1])
                g[(pl.ds(start + half, half), *where)] = jnp.where(low, turned[0], parts[1])


def solve(k, kind, values, shift):
    shape = values.shape
    flat = values.reshape(shape[0] * shape[1], shape[2])
    spectrum = dot(k["spectrum_rows"][...], dot(flat, k["spectrum_lanes"][...]))
    spectrum = spectrum / (k["eigen"][...] + shift)
    fine = dot(k[kind + "_rows2"][...], dot(spectrum, k[kind + "_lanes2"][...]))
    return fine.reshape(shape)


def cycle2(k, v, g, shift):
    weight = 0.25**2
    diagonal = 6.0 * weight + shift
    damp = DAMPING / diagonal
    if v is None:
        v = damp * g
    else:
        v = v + damp * (g - (diagonal * v - weight * around_all(v)))
    v = v + solve(k, "linear", g - (diagonal * v - weight * around_all(v)), shift)
    return v + damp * (g - (diagonal * v - weight * around_all(v)))


def down(k, t, shape2):
    flat = row_blocks(k["down_rows"][...], t[...].reshape(-1, t.shape[2]), 3)
    return right(flat, k["down_lanes"][...], 3).reshape(shape2)


def up(k, kind, level, values, z):
    flat = right(values, k[kind + "_lanes" + level][...], 2)
    z[...] = row_blocks(k[kind + "_rows" + level][...], flat, 2).reshape(z.shape)


def blend(z, i, weights, count):
    total = None
    for offset, weight in weights.items():
        index = i + offset
        index = index if count is None else lax.rem(index + count, count)
        term = weight * z[index]
        total = term if total is None else total + term
    return total


def up1(k, kind, values, z, v, add):
    count = z.shape[0]
    up(k, kind, "1", values.reshape(-1, values.shape[2]), z)
    weights = CUBIC if kind == "cubic" else LINEAR

    def body(i):
        for odd in (0, 1):
            p = 2 * i + odd + 1
            value = blend(z, i, weights[odd], count)
            v[p] = v[p] + value if add else value

    loop(count, body)
    close(v)


def cycle1(k, v, u, g, t, z, shift, zero, shape2):
    weight = 0.25
    diagonal = 6.0 * weight + shift
    damp = DAMPING / diagonal
    count = g.shape[0]

    def before(p):
        if zero:
            u[p + 1] = damp * g[p]
        else:
            center, rest = defect_plane(v, p + 1, g[p], weight, diagonal)
            u[p + 1] = center + damp * rest

    loop(count, before)
    close(u)

    def residue(i):
        t[i] = (
            defect_plane(u, 2 * i + 1, g[2 * i], weight, diagonal)[1]
            + defect_plane(u, 2 * i + 2, g[2 * i + 1], weight, diagonal)[1]
        )

    loop(count // 2, residue)
    correction = cycle2(k, None, down(k, t, shape2), shift)
    up1(k, "linear", correction, z, u, True)

    def after(p):
        center, rest = defect_plane(u, p + 1, g[p], weight, diagonal)
        v[p + 1] = center + damp * rest

    loop(count, after)
    close(v)


def window(k, kind, v, zw, span, write):
    count = v.shape[0] - 2
    values = jnp.concatenate([v[count - 3 : count + 1], v[1 : span - 3]], axis=0)
    up(k, kind, "0", values.reshape(-1, values.shape[2]), zw)
    weights = CUBIC if kind == "cubic" else LINEAR

    def body(i):
        for odd in (0, 1):
            write(2 * i + odd, blend(zw, i + 3, weights[odd], None))

    loop(span - 6, body)


def own_defect(v, p, f, weight, diagonal):
    rows, lanes = f.shape
    inside = (pl.ds(8, rows), pl.ds(lanes, lanes))
    wide = v[p + 1, pl.ds(8, rows), :]
    center = wide[:, lanes:]
    beside = v[(p, *inside)] + v[(p + 2, *inside)]
    beside = beside + v[p + 1, pl.ds(7, rows), pl.ds(lanes, lanes)]
    beside = beside + v[p + 1, pl.ds(9, rows), pl.ds(lanes, lanes)]
    beside = beside + pltpu.roll(wide, 1, 1)[:, lanes:]
    beside = beside + pltpu.roll(wide, 2 * lanes - 1, 1)[:, lanes:]
    return center, f - (diagonal * center - weight * beside)


def position():
    return tuple(lax.axis_index(name) for name in NAMES)


def partner_of(place):
    x, y, z = place
    return (x, y + 1 - 2 * lax.rem(y, 2), z)


def shifted(place, counts, offset):
    return tuple(
        lax.rem(at + step + count, count) for at, step, count in zip(place, offset, counts)
    )


def slot(place, counts):
    return (place[0] * counts[1] + place[1]) * counts[2] + place[2]


def chip_offsets(counts):
    nx, ny, nz = counts
    offsets = [
        (dx, dy, dz) for dx in range(nx) for dy in range(0, ny, 2) for dz in range(nz)
    ]

    def hops(offset):
        return sum(min(step, count - step) for step, count in zip(offset, (nx, ny, nz)))

    return sorted(offsets[1:], key=hops, reverse=True)


def face_offsets(counts):
    faces = []
    for axis in range(3):
        for side, step in ((0, -1), (1, 1)):
            offset = [0, 0, 0]
            offset[axis] = step
            faces.append((tuple(offset), axis, side))
    return faces


def greet(barrier, places):
    for place in places:
        pl.semaphore_signal(barrier, inc=1, device_id=place, device_id_type=MESH)


def remote(src, dst, send, recv, place):
    return pltpu.make_async_remote_copy(
        src_ref=src, dst_ref=dst, send_sem=send, recv_sem=recv, device_id=place, device_id_type=MESH
    )


def spread(counts, block, gathered, sems):
    send, recv, relay_send, relay_recv = sems
    me = position()
    partner = partner_of(me)
    offsets = chip_offsets(counts)
    mine = gathered.at[slot(me, counts)]
    copies = []
    for n, offset in enumerate(offsets):
        place = shifted(me, counts, offset)
        copies.append(remote(block, mine, send.at[n], recv.at[n], place))
        copies[-1].start()
    last = len(offsets)
    relays = [remote(block, mine, relay_send.at[last], relay_recv.at[last], partner)]
    relays[0].start()

    def finish():
        gathered[slot(me, counts)] = block[...]
        for n, offset in reversed(list(enumerate(offsets))):
            copies[n].wait_recv()
            source = shifted(me, counts, tuple(-step for step in offset))
            arrived = gathered.at[slot(source, counts)]
            relays.append(
                remote(arrived, arrived, relay_send.at[n], relay_recv.at[n], partner)
            )
            relays[-1].start()
        for copy in copies:
            copy.wait_send()
        for relay in relays:
            relay.wait()

    return finish


def gather_places(counts):
    me = position()
    return [shifted(me, counts, offset) for offset in chip_offsets(counts)] + [partner_of(me)]


def first_part(k, counts, source, f, gathered, halos, block, owns, sems, face_sems):
    own_planes, own_rows, own_columns = owns
    planes, rows, columns = halos
    face_send, face_recv = face_sems
    me = position()
    barrier = pltpu.get_barrier_semaphore()
    faces = face_offsets(counts)
    places = gather_places(counts) + [shifted(me, counts, offset) for offset, _, _ in faces]
    greet(barrier, places)
    b0, b1, b2 = source.shape
    summed = source[...].reshape(b0 // 2, 2, b1, b2)
    block[...] = restrict_own(k, summed[:, 0] + summed[:, 1]).reshape(block.shape)
    own_planes[0] = source[0]
    own_planes[1] = source[b0 - 1]
    own_rows[0] = source[:, pl.ds(0, 1), :]
    own_rows[1] = source[:, pl.ds(b1 - 1, 1), :]
    turned = source[...].reshape(b0 * b1, b2).T
    own_columns[0] = turned[:8]
    own_columns[1] = turned[b2 - 8 :]
    pl.semaphore_wait(barrier, len(places))
    finish = spread(counts, block, gathered, sems)
    buffers = ((own_planes, planes), (own_rows, rows), (own_columns, columns))
    order = (0, 2, 1)
    copies = []
    for n, (offset, axis, side) in enumerate(faces):
        own, halo = buffers[order[axis]]
        place = shifted(me, counts, offset)
        copies.append(
            remote(own.at[side], halo.at[1 - side], face_send.at[n], face_recv.at[n], place)
        )
        copies[-1].start()
    f[...] = jnp.zeros_like(f)
    f[1 : b0 + 1, pl.ds(8, b1), pl.ds(b2, b2)] = source[...]
    finish()
    for copy in copies:
        copy.wait()


def second_part(k, counts, shape2, span, shift, gathered, source, halos, out, buffers):
    g, v, u, t, z, zw, v0, v1, f, summed = buffers
    plane_halo, row_halo, column_halo = halos
    unpack(gathered, counts, g)
    b0, b1, b2 = source.shape
    rows, lanes = pl.ds(8, b1), pl.ds(b2, b2)
    f[0, rows, lanes] = plane_halo[0]
    f[b0 + 1, rows, lanes] = plane_halo[1]
    f[1 : b0 + 1, pl.ds(7, 1), lanes] = row_halo[0]
    f[1 : b0 + 1, pl.ds(8 + b1, 1), lanes] = row_halo[1]
    middle = jnp.zeros((b2 - 16, b0 * b1), jnp.float32)
    turned = jnp.concatenate([column_halo[1], middle, column_halo[0]], axis=0)
    f[1 : b0 + 1, rows, pl.ds(0, b2)] = turned.T.reshape(b0, b1, b2)
    def pair_sum(i):
        t[i] = g[2 * i] + g[2 * i + 1]

    loop(g.shape[0] // 2, pair_sum)
    forcing2 = down(k, t, shape2)
    iterate2 = cycle2(k, solve(k, "cubic", forcing2, shift), forcing2, shift)
    up1(k, "cubic", iterate2, z, v, False)
    cycle1(k, v, u, g, t, z, shift, False, shape2)

    def put(p, value):
        v0[p] = value

    window(k, "cubic", v, zw, span, put)
    diagonal = 6.0 + shift
    damp = DAMPING / diagonal

    def before(p):
        center, rest = defect_plane(v0, p + 1, f[p], 1.0, diagonal)
        v1[p] = center + damp * rest

    loop(b0 + 2, before)

    def residue(i):
        summed[i] = (
            own_defect(v1, 2 * i, source[2 * i], 1.0, diagonal)[1]
            + own_defect(v1, 2 * i + 1, source[2 * i + 1], 1.0, diagonal)[1]
        )

    loop(b0 // 2, residue)
    out[...] = restrict_own(k, summed[...]).reshape(out.shape)


def third_part(k, counts, shape2, span, shift, gathered, source, out, buffers):
    g, v, u, t, z, zw, w, v1 = buffers[:8]
    unpack(gathered, counts, g)
    cycle1(k, v, u, g, t, z, shift, True, shape2)
    b0 = source.shape[0]

    def put(p, value):
        w[p] = value

    window(k, "linear", v, zw, span, put)

    def add(p):
        w[p] = v1[p] + w[p + 1]

    loop(b0 + 2, add)
    diagonal = 6.0 + shift
    damp = DAMPING / diagonal

    def after(p):
        center, rest = own_defect(w, p, source[p], 1.0, diagonal)
        out[p] = center + damp * rest

    loop(b0, after)


def kernel(names, counts, shape2, span, *refs):
    k = dict(zip(names, refs))
    shift_ref, source, out, *rest = refs[len(names) :]
    shift = shift_ref[0]
    landing, later, *halos = rest[:5]
    block, block_later, *owns = rest[5:10]
    buffers = rest[10:20]
    sems, sems_later, face_sems = rest[20:24], rest[24:28], rest[28:30]
    f = buffers[8]
    first_part(k, counts, source, f, landing, halos, block, owns, sems, face_sems)
    second_part(k, counts, shape2, span, shift, landing, source, halos, block_later, buffers)
    spread(counts, block_later, later, sems_later)()
    third_part(k, counts, shape2, span, shift, later, source, out, buffers)


def per_device(counts, source, shift):
    nx, ny, nz = counts
    b0, b1, b2 = source.shape
    sizes = (b0 * nx, b1 * nz, b2 * ny)
    table = constants(source.shape, sizes)
    m0, m1, m2 = (size // 2 for size in sizes)
    shape2 = tuple(size // 4 for size in sizes)
    span = b0 // 2 + 8
    wide = (b1 + 16, 2 * b2)
    packed = (b0 // 4, b1 // 2, b2)
    devices = nx * ny * nz
    chips = devices // 2
    vmem = pl.BlockSpec(memory_space=pltpu.VMEM)

    def field(*shape):
        return pltpu.VMEM(shape, jnp.float32)

    faces = [field(2, b1, b2), field(2, b0, 1, b2), field(2, 8, b0 * b1)]
    buffers = [
        field(m0, m1, m2),
        field(m0 + 2, m1, m2),
        field(m0 + 2, m1, m2),
        field(m0 // 2, m1, m2),
        field(m0 // 2, m1, m2),
        field(span, *wide),
        field(b0 + 4, *wide),
        field(b0 + 2, *wide),
        field(b0 + 2, *wide),
        field(b0 // 2, b1, b2),
    ]
    sems = [pltpu.SemaphoreType.DMA((max(chips - 1, 1),))] * 2
    sems += [pltpu.SemaphoreType.DMA((chips,))] * 2
    landing = [field(devices, *packed)] * 2 + faces
    names = tuple(table)
    return pl.pallas_call(
        functools.partial(kernel, names, counts, shape2, span),
        out_shape=jax.ShapeDtypeStruct(source.shape, jnp.float32),
        in_specs=[vmem] * len(names) + [pl.BlockSpec(memory_space=pltpu.SMEM), vmem],
        out_specs=vmem,
        scratch_shapes=landing
        + [field(*packed)] * 2
        + faces
        + buffers
        + sems * 2
        + [pltpu.SemaphoreType.DMA((6,))] * 2,
        compiler_params=pltpu.CompilerParams(
            vmem_limit_bytes=60 * 1024 * 1024, collective_id=0, has_side_effects=True
        ),
    )(*[jnp.asarray(table[name]) for name in names], shift, source)


def solution(mesh):
    counts = tuple(mesh.shape[name] for name in NAMES)
    return jax.shard_map(
        functools.partial(per_device, counts),
        mesh=mesh,
        in_specs=(P("gx", "gz", "gy"), P()),
        out_specs=P("gx", "gz", "gy"),
        check_vma=False,
    )
```

```python
import functools

import jax
import jax.numpy as jnp
import numpy as np
from jax import lax
from jax.experimental import pallas as pl
from jax.experimental.pallas import tpu as pltpu
from jax.sharding import PartitionSpec as P

LEVELS = 4
DAMPING = 6.0 / 7.0
PRECISE = lax.Precision.HIGHEST
CUBIC = (
    {-2: -5.0 / 128.0, -1: 35.0 / 128.0, 0: 105.0 / 128.0, 1: -7.0 / 128.0},
    {-1: -7.0 / 128.0, 0: 105.0 / 128.0, 1: 35.0 / 128.0, 2: -5.0 / 128.0},
)
LINEAR = ({-1: 0.25, 0: 0.75}, {0: 0.75, 1: 0.25})
NAMES = ("gx", "gy", "gz")
MESH = pl.DeviceIdType.MESH


def basis(count):
    cells = np.arange(count)
    columns, cosines = [], []
    for m in range(count):
        k = (m + 1) // 2
        angle = 2.0 * np.pi * k * cells / count
        column = np.cos(angle) if m % 2 == 1 or m == 0 else np.sin(angle)
        columns.append(column / np.sqrt(np.sum(column**2)))
        cosines.append(np.cos(2.0 * np.pi * k / count))
    return np.stack(columns, axis=1), np.array(cosines, np.float32)


def interpolation(coarse_count, fine_cells, weights):
    matrix = np.zeros((len(fine_cells), coarse_count))
    for row, cell in enumerate(fine_cells):
        for offset, weight in weights[cell % 2].items():
            matrix[row, (cell // 2 + offset) % coarse_count] += weight
    return matrix


def pairs(coarse_count):
    return np.kron(np.eye(coarse_count), np.ones((1, 2)))


def blocked(matrix):
    count = max(1, 128 // matrix.shape[1])
    return np.kron(np.eye(count), matrix)


def constants(block, sizes):
    b0, b1, b2 = block
    m0, m1, m2 = (size // 2 for size in sizes)
    q0, q1, q2 = (size // 4 for size in sizes)
    c0, c1, c2 = (size // 8 for size in sizes)
    table = {}
    table["own_rows"] = np.kron(np.eye(b0 // 2), pairs(b1 // 2))
    lanes = 0.125 * pairs(b2 // 2).T
    table["own_lo"] = np.concatenate([lanes, np.zeros_like(lanes)], axis=1)
    table["own_hi"] = np.concatenate([np.zeros_like(lanes), lanes], axis=1)
    table["down_rows"] = blocked(pairs(q1))
    table["down_lanes"] = 0.125 * pairs(q2).T
    window_lanes = [b2 + j for j in range(b2 // 2)] + [j - b2 for j in range(b2 // 2, 2 * b2)]
    window_rows = [j - 8 for j in range(b1 + 16)]
    for name, weights in (("cubic", CUBIC), ("linear", LINEAR)):
        table[name + "_rows1"] = blocked(interpolation(q1, range(m1), weights))
        table[name + "_lanes1"] = interpolation(q2, range(m2), weights).T
        table[name + "_rows0"] = blocked(interpolation(m1, window_rows, weights))
        table[name + "_lanes0"] = interpolation(m2, window_lanes, weights).T
    (u0, cos0), (u1, cos1), (u2, cos2) = basis(c0), basis(c1), basis(c2)
    table["spectrum_rows"] = np.kron(u0.T @ pairs(c0), u1.T @ pairs(c1))
    table["spectrum_lanes"] = 0.125 * pairs(c2).T @ u2
    for name, weights in (("cubic", CUBIC), ("linear", LINEAR)):
        table[name + "_rows2"] = np.kron(
            interpolation(c0, range(q0), weights) @ u0, interpolation(c1, range(q1), weights) @ u1
        )
        table[name + "_lanes2"] = u2.T @ interpolation(c2, range(q2), weights).T
    two = np.float32(2.0)
    eigen = (
        np.float32(6.0)
        - two * cos0[:, None, None]
        - two * cos1[None, :, None]
        - two * cos2[None, None, :]
    )
    table["eigen"] = (np.float32(0.25 ** (LEVELS - 1)) * eigen).reshape(c0 * c1, c2)
    wide = ("spectrum_rows", "spectrum_lanes", "eigen")
    return {
        name: np.asarray(
            value, np.float32 if name in wide or name.endswith("2") else jnp.bfloat16
        )
        for name, value in table.items()
    }


def dot(a, b):
    return jnp.dot(a, b, precision=PRECISE, preferred_element_type=jnp.float32)


def parts_of(values, pieces):
    parts = []
    for n in range(pieces):
        parts.append(values.astype(jnp.bfloat16))
        if n + 1 < pieces:
            values = values - parts[-1].astype(jnp.float32)
    return parts[::-1]


def right(values, matrix, pieces):
    terms = [
        jnp.dot(part, matrix, preferred_element_type=jnp.float32)
        for part in parts_of(values, pieces)
    ]
    return sum(terms[1:], terms[0])


def left(matrix, values, pieces):
    terms = [
        jnp.dot(matrix, part, preferred_element_type=jnp.float32)
        for part in parts_of(values, pieces)
    ]
    return sum(terms[1:], terms[0])


def around(plane):
    rows, lanes = plane.shape
    total = pltpu.roll(plane, 1, 0) + pltpu.roll(plane, rows - 1, 0)
    return total + (pltpu.roll(plane, 1, 1) + pltpu.roll(plane, lanes - 1, 1))


def around_all(values):
    first = jnp.concatenate([values[1:], values[:1]], axis=0)
    first = first + jnp.concatenate([values[-1:], values[:-1]], axis=0)
    for axis in (1, 2):
        first = first + pltpu.roll(values, 1, axis)
        first = first + pltpu.roll(values, values.shape[axis] - 1, axis)
    return first


def row_blocks(matrix, values, pieces):
    depth = matrix.shape[1]
    return jnp.concatenate(
        [left(matrix, values[i : i + depth], pieces) for i in range(0, values.shape[0], depth)], axis=0
    )


def loop(count, body):
    def step(i, carry):
        body(i)
        return carry

    lax.fori_loop(0, count, step, 0, unroll=4 if count % 4 == 0 else 2)


def close(ref):
    count = ref.shape[0] - 2
    ref[0] = ref[count]
    ref[count + 1] = ref[1]


def defect_plane(v, p, g, weight, diagonal):
    center = v[p]
    beside = v[p - 1] + v[p + 1] + around(center)
    return center, g - (diagonal * center - weight * beside)


def restrict_own(k, summed):
    b_half, rows, lanes = summed.shape
    folded = left(k["own_rows"][...], summed.reshape(b_half * rows, lanes), 3)
    half = folded.shape[0] // 2
    return right(folded[:half], k["own_lo"][...], 3) + right(folded[half:], k["own_hi"][...], 3)


def unpack(gathered, counts, g):
    nx, ny, nz = counts
    x, y, z = (lax.axis_index(name) for name in NAMES)
    half, rows, lanes = gathered.shape[1:]
    low = lax.broadcasted_iota(jnp.int32, (half, rows, lanes), 2) < lanes // 2
    for dx in range(nx):
        for dz in range(nz):
            for pair in range(ny // 2):
                parts = []
                for dy in (2 * pair, 2 * pair + 1):
                    index = (lax.rem(x + dx, nx) * ny + lax.rem(y + dy, ny)) * nz
                    parts.append(gathered[index + lax.rem(z + dz, nz)])
                turned = [pltpu.roll(part, lanes // 2, 2) for part in parts]
                where = (pl.ds(dz * rows, rows), pl.ds(pair * lanes, lanes))
                start = 2 * half * dx
                g[(pl.ds(start, half), *where)] = jnp.where(low, parts[0], turned[1])
                g[(pl.ds(start + half, half), *where)] = jnp.where(low, turned[0], parts[1])


def solve(k, kind, values, shift):
    shape = values.shape
    flat = values.reshape(shape[0] * shape[1], shape[2])
    spectrum = dot(k["spectrum_rows"][...], dot(flat, k["spectrum_lanes"][...]))
    spectrum = spectrum / (k["eigen"][...] + shift)
    fine = dot(k[kind + "_rows2"][...], dot(spectrum, k[kind + "_lanes2"][...]))
    return fine.reshape(shape)


def cycle2(k, v, g, shift):
    weight = 0.25**2
    diagonal = 6.0 * weight + shift
    damp = DAMPING / diagonal
    if v is None:
        v = damp * g
    else:
        v = v + damp * (g - (diagonal * v - weight * around_all(v)))
    v = v + solve(k, "linear", g - (diagonal * v - weight * around_all(v)), shift)
    return v + damp * (g - (diagonal * v - weight * around_all(v)))


def down(k, t, shape2):
    flat = row_blocks(k["down_rows"][...], t[...].reshape(-1, t.shape[2]), 3)
    return right(flat, k["down_lanes"][...], 3).reshape(shape2)


def up(k, kind, level, values, z):
    flat = right(values, k[kind + "_lanes" + level][...], 2)
    z[...] = row_blocks(k[kind + "_rows" + level][...], flat, 2).reshape(z.shape)


def blend(z, i, weights, count):
    total = None
    for offset, weight in weights.items():
        index = i + offset
        index = index if count is None else lax.rem(index + count, count)
        term = weight * z[index]
        total = term if total is None else total + term
    return total


def up1(k, kind, values, z, v, add):
    count = z.shape[0]
    up(k, kind, "1", values.reshape(-1, values.shape[2]), z)
    weights = CUBIC if kind == "cubic" else LINEAR

    def body(i):
        for odd in (0, 1):
            p = 2 * i + odd + 1
            value = blend(z, i, weights[odd], count)
            v[p] = v[p] + value if add else value

    loop(count, body)
    close(v)


def cycle1(k, v, u, g, t, z, shift, zero, shape2):
    weight = 0.25
    diagonal = 6.0 * weight + shift
    damp = DAMPING / diagonal
    count = g.shape[0]

    def before(p):
        if zero:
            u[p + 1] = damp * g[p]
        else:
            center, rest = defect_plane(v, p + 1, g[p], weight, diagonal)
            u[p + 1] = center + damp * rest

    loop(count, before)
    close(u)

    def residue(i):
        t[i] = (
            defect_plane(u, 2 * i + 1, g[2 * i], weight, diagonal)[1]
            + defect_plane(u, 2 * i + 2, g[2 * i + 1], weight, diagonal)[1]
        )

    loop(count // 2, residue)
    correction = cycle2(k, None, down(k, t, shape2), shift)
    up1(k, "linear", correction, z, u, True)

    def after(p):
        center, rest = defect_plane(u, p + 1, g[p], weight, diagonal)
        v[p + 1] = center + damp * rest

    loop(count, after)
    close(v)


def window(k, kind, v, zw, span, write):
    count = v.shape[0] - 2
    values = jnp.concatenate([v[count - 3 : count + 1], v[1 : span - 3]], axis=0)
    up(k, kind, "0", values.reshape(-1, values.shape[2]), zw)
    weights = CUBIC if kind == "cubic" else LINEAR

    def body(i):
        for odd in (0, 1):
            write(2 * i + odd, blend(zw, i + 3, weights[odd], None))

    loop(span - 6, body)


def own_defect(v, p, f, weight, diagonal):
    rows, lanes = f.shape
    inside = (pl.ds(8, rows), pl.ds(lanes, lanes))
    wide = v[p + 1, pl.ds(8, rows), :]
    center = wide[:, lanes:]
    beside = v[(p, *inside)] + v[(p + 2, *inside)]
    beside = beside + v[p + 1, pl.ds(7, rows), pl.ds(lanes, lanes)]
    beside = beside + v[p + 1, pl.ds(9, rows), pl.ds(lanes, lanes)]
    beside = beside + pltpu.roll(wide, 1, 1)[:, lanes:]
    beside = beside + pltpu.roll(wide, 2 * lanes - 1, 1)[:, lanes:]
    return center, f - (diagonal * center - weight * beside)


def position():
    return tuple(lax.axis_index(name) for name in NAMES)


def partner_of(place):
    x, y, z = place
    return (x, y + 1 - 2 * lax.rem(y, 2), z)


def shifted(place, counts, offset):
    return tuple(
        lax.rem(at + step + count, count) for at, step, count in zip(place, offset, counts)
    )


def slot(place, counts):
    return (place[0] * counts[1] + place[1]) * counts[2] + place[2]


def chip_offsets(counts):
    nx, ny, nz = counts
    offsets = [
        (dx, dy, dz) for dx in range(nx) for dy in range(0, ny, 2) for dz in range(nz)
    ]

    def hops(offset):
        return sum(min(step, count - step) for step, count in zip(offset, (nx, ny, nz)))

    return sorted(offsets[1:], key=hops, reverse=True)


def face_offsets(counts):
    faces = []
    for axis in range(3):
        for side, step in ((0, -1), (1, 1)):
            offset = [0, 0, 0]
            offset[axis] = step
            faces.append((tuple(offset), axis, side))
    return faces


def greet(barrier, places):
    for place in places:
        pl.semaphore_signal(barrier, inc=1, device_id=place, device_id_type=MESH)


def remote(src, dst, send, recv, place):
    return pltpu.make_async_remote_copy(
        src_ref=src, dst_ref=dst, send_sem=send, recv_sem=recv, device_id=place, device_id_type=MESH
    )


def spread(counts, block, gathered, sems):
    send, recv, relay_send, relay_recv = sems
    me = position()
    partner = partner_of(me)
    along, across = stages(counts)
    number = {offset: n for n, offset in enumerate(chip_offsets(counts))}
    mine = gathered.at[slot(me, counts)]
    copies, relays = {}, []

    def pass_on(offset, source, target, place):
        n = number[offset]
        copies[offset] = remote(source, target, send.at[n], recv.at[n], place)
        copies[offset].start()

    def relay(n, source, target):
        relays.append(remote(source, target, relay_send.at[n], relay_recv.at[n], partner))
        relays[-1].start()

    for offset in along + across:
        pass_on(offset, block, mine, shifted(me, counts, offset))
    relay(len(number), block, mine)

    def arrival(offset):
        copies[offset].wait_recv()
        source = shifted(me, counts, tuple(-step for step in offset))
        return gathered.at[slot(source, counts)]

    def finish():
        gathered[slot(me, counts)] = block[...]
        for first in along[::-1]:
            arrived = arrival(first)
            for second in across:
                place = shifted(me, counts, second)
                pass_on((first[0], second[1], second[2]), arrived, arrived, place)
            relay(number[first], arrived, arrived)
        for first in ((0, 0, 0), *along[::-1]):
            for second in across[::-1]:
                offset = (first[0], second[1], second[2])
                arrived = arrival(offset)
                relay(number[offset], arrived, arrived)
        for copy in copies.values():
            copy.wait_send()
        for copy in relays:
            copy.wait()

    return finish


def stages(counts):
    offsets = chip_offsets(counts)
    along = [offset for offset in offsets if offset[1:] == (0, 0)]
    across = [offset for offset in offsets if offset[0] == 0]
    return along, across


def gather_places(counts):
    me = position()
    along, across = stages(counts)
    return [shifted(me, counts, offset) for offset in along + across] + [partner_of(me)]


def first_part(k, counts, source, f, gathered, halos, block, owns, sems, face_sems):
    own_planes, own_rows, own_columns = owns
    planes, rows, columns = halos
    face_send, face_recv = face_sems
    me = position()
    barrier = pltpu.get_barrier_semaphore()
    faces = face_offsets(counts)
    places = gather_places(counts) + [shifted(me, counts, offset) for offset, _, _ in faces]
    greet(barrier, places)
    b0, b1, b2 = source.shape
    summed = source[...].reshape(b0 // 2, 2, b1, b2)
    block[...] = restrict_own(k, summed[:, 0] + summed[:, 1]).reshape(block.shape)
    own_planes[0] = source[0]
    own_planes[1] = source[b0 - 1]
    own_rows[0] = source[:, pl.ds(0, 1), :]
    own_rows[1] = source[:, pl.ds(b1 - 1, 1), :]
    turned = source[...].reshape(b0 * b1, b2).T
    own_columns[0] = turned[:8]
    own_columns[1] = turned[b2 - 8 :]
    pl.semaphore_wait(barrier, len(places))
    finish = spread(counts, block, gathered, sems)
    buffers = ((own_planes, planes), (own_rows, rows), (own_columns, columns))
    order = (0, 2, 1)
    copies = []
    for n, (offset, axis, side) in enumerate(faces):
        own, halo = buffers[order[axis]]
        place = shifted(me, counts, offset)
        copies.append(
            remote(own.at[side], halo.at[1 - side], face_send.at[n], face_recv.at[n], place)
        )
        copies[-1].start()
    f[...] = jnp.zeros_like(f)
    f[1 : b0 + 1, pl.ds(8, b1), pl.ds(b2, b2)] = source[...]
    finish()
    for copy in copies:
        copy.wait()


def second_part(k, counts, shape2, span, shift, gathered, source, halos, out, buffers):
    g, v, u, t, z, zw, v0, v1, f, summed = buffers
    plane_halo, row_halo, column_halo = halos
    unpack(gathered, counts, g)
    b0, b1, b2 = source.shape
    rows, lanes = pl.ds(8, b1), pl.ds(b2, b2)
    f[0, rows, lanes] = plane_halo[0]
    f[b0 + 1, rows, lanes] = plane_halo[1]
    f[1 : b0 + 1, pl.ds(7, 1), lanes] = row_halo[0]
    f[1 : b0 + 1, pl.ds(8 + b1, 1), lanes] = row_halo[1]
    middle = jnp.zeros((b2 - 16, b0 * b1), jnp.float32)
    turned = jnp.concatenate([column_halo[1], middle, column_halo[0]], axis=0)
    f[1 : b0 + 1, rows, pl.ds(0, b2)] = turned.T.reshape(b0, b1, b2)
    def pair_sum(i):
        t[i] = g[2 * i] + g[2 * i + 1]

    loop(g.shape[0] // 2, pair_sum)
    forcing2 = down(k, t, shape2)
    iterate2 = cycle2(k, solve(k, "cubic", forcing2, shift), forcing2, shift)
    up1(k, "cubic", iterate2, z, v, False)
    cycle1(k, v, u, g, t, z, shift, False, shape2)

    def put(p, value):
        v0[p] = value

    window(k, "cubic", v, zw, span, put)
    diagonal = 6.0 + shift
    damp = DAMPING / diagonal

    def before(p):
        center, rest = defect_plane(v0, p + 1, f[p], 1.0, diagonal)
        v1[p] = center + damp * rest

    loop(b0 + 2, before)

    def residue(i):
        summed[i] = (
            own_defect(v1, 2 * i, source[2 * i], 1.0, diagonal)[1]
            + own_defect(v1, 2 * i + 1, source[2 * i + 1], 1.0, diagonal)[1]
        )

    loop(b0 // 2, residue)
    out[...] = restrict_own(k, summed[...]).reshape(out.shape)


def third_part(k, counts, shape2, span, shift, gathered, source, out, buffers):
    g, v, u, t, z, zw, w, v1 = buffers[:8]
    unpack(gathered, counts, g)
    cycle1(k, v, u, g, t, z, shift, True, shape2)
    b0 = source.shape[0]

    def put(p, value):
        w[p] = value

    window(k, "linear", v, zw, span, put)

    def add(p):
        w[p] = v1[p] + w[p + 1]

    loop(b0 + 2, add)
    diagonal = 6.0 + shift
    damp = DAMPING / diagonal

    def after(p):
        center, rest = own_defect(w, p, source[p], 1.0, diagonal)
        out[p] = center + damp * rest

    loop(b0, after)


def kernel(names, counts, shape2, span, *refs):
    k = dict(zip(names, refs))
    shift_ref, source, out, *rest = refs[len(names) :]
    shift = shift_ref[0]
    landing, later, *halos = rest[:5]
    block, block_later, *owns = rest[5:10]
    buffers = rest[10:20]
    sems, sems_later, face_sems = rest[20:24], rest[24:28], rest[28:30]
    f = buffers[8]
    first_part(k, counts, source, f, landing, halos, block, owns, sems, face_sems)
    second_part(k, counts, shape2, span, shift, landing, source, halos, block_later, buffers)
    spread(counts, block_later, later, sems_later)()
    third_part(k, counts, shape2, span, shift, later, source, out, buffers)


def per_device(counts, source, shift):
    nx, ny, nz = counts
    b0, b1, b2 = source.shape
    sizes = (b0 * nx, b1 * nz, b2 * ny)
    table = constants(source.shape, sizes)
    m0, m1, m2 = (size // 2 for size in sizes)
    shape2 = tuple(size // 4 for size in sizes)
    span = b0 // 2 + 8
    wide = (b1 + 16, 2 * b2)
    packed = (b0 // 4, b1 // 2, b2)
    devices = nx * ny * nz
    chips = devices // 2
    vmem = pl.BlockSpec(memory_space=pltpu.VMEM)

    def field(*shape):
        return pltpu.VMEM(shape, jnp.float32)

    faces = [field(2, b1, b2), field(2, b0, 1, b2), field(2, 8, b0 * b1)]
    buffers = [
        field(m0, m1, m2),
        field(m0 + 2, m1, m2),
        field(m0 + 2, m1, m2),
        field(m0 // 2, m1, m2),
        field(m0 // 2, m1, m2),
        field(span, *wide),
        field(b0 + 4, *wide),
        field(b0 + 2, *wide),
        field(b0 + 2, *wide),
        field(b0 // 2, b1, b2),
    ]
    sems = [pltpu.SemaphoreType.DMA((max(chips - 1, 1),))] * 2
    sems += [pltpu.SemaphoreType.DMA((chips,))] * 2
    landing = [field(devices, *packed)] * 2 + faces
    names = tuple(table)
    return pl.pallas_call(
        functools.partial(kernel, names, counts, shape2, span),
        out_shape=jax.ShapeDtypeStruct(source.shape, jnp.float32),
        in_specs=[vmem] * len(names) + [pl.BlockSpec(memory_space=pltpu.SMEM), vmem],
        out_specs=vmem,
        scratch_shapes=landing
        + [field(*packed)] * 2
        + faces
        + buffers
        + sems * 2
        + [pltpu.SemaphoreType.DMA((6,))] * 2,
        compiler_params=pltpu.CompilerParams(
            vmem_limit_bytes=60 * 1024 * 1024, collective_id=0, has_side_effects=True
        ),
    )(*[jnp.asarray(table[name]) for name in names], shift, source)


def solution(mesh):
    counts = tuple(mesh.shape[name] for name in NAMES)
    return jax.shard_map(
        functools.partial(per_device, counts),
        mesh=mesh,
        in_specs=(P("gx", "gz", "gy"), P()),
        out_specs=P("gx", "gz", "gy"),
        check_vma=False,
    )
```
